32 devices in a mesh: blk: 16 (over z, x, core), col: 2 (over y).
Axes of the slice: x: 2, y: 2, z: 4, core: 2. Of those that a mesh axis runs over, the one named last changes fastest.
Arguments:
- features: bfloat16 [4096, 128], P(('blk', 'col')), may hold values from -600 to 600
- tile_vals: bfloat16 [16, 128, 256, 256], P('blk', None, 'col'), may hold values from -8 to 8, as said below
- tile_cols: int32 [16, 128], P('blk'), may hold values from 0 to 15
- tile_count: int32 [16], P('blk'), may hold values from 32 to 128, as said below
- norm_gain: float32 [3, 128], replicated, may hold values from 0.25 to 1.75
Outputs:
- propagated: bfloat16 [4096, 128], P(('blk', 'col'))
The draws below stay inside these ranges and needn't reach their ends.
Inputs may be any that keep to these rules, and one draw needn't show every extreme that they name: `tile_vals`: adjacency tiles are sparse: most entries are zero. `tile_count`: slots at or past a row block's count hold no tile; some row block has exactly 128 live slots in every draw. `tile_cols`: live slots of one row block may name the same column block more than once; entries of dead slots carry no meaning.
All inputs are finite; a program needn't handle non-finite values.
Results may differ from the reference program's by a relative error of at most 0.0052.
Values may be sent and summed in bfloat16 or wider, within the bound.
No kernel may reach another device: no remote copies, remote signals or barrier semaphores. Data moves between devices by JAX's collectives and lax.ppermute only.
A program may use at most 128 MiB of HBM per device.

```python
import jax
import jax.numpy as jnp
from jax import lax

WIDTH = 128
TILE = 256
TILE_CAP = 128
HOPS = 3
BLOCKS = 16
NODES = 4096


def draw_features(key, part):
    key_values, key_rows = jax.random.split(jax.random.fold_in(key, 11))
    column_pos = jnp.arange(WIDTH, dtype=jnp.float32) / (WIDTH - 1)
    normal_part = jnp.clip(jax.random.normal(key_values, (NODES, WIDTH), jnp.float32), -6.0, 6.0)
    col_scale = 10.0 ** column_pos
    row_scale = 10.0 ** jax.random.uniform(key_rows, (NODES, 1), jnp.float32)
    return (normal_part * row_scale * col_scale[None, :]).astype(jnp.bfloat16)


def draw_tile_vals(key, part):
    density = min(1.0, 8.0 / TILE)
    spread = (TILE_CAP * TILE * density / 2.0) ** (-0.5)
    base_key = jax.random.fold_in(key, 37)

    def one_block(block_index):
        key_block = jax.random.fold_in(base_key, block_index)
        key_values, key_mask = jax.random.split(key_block)
        values = jnp.clip(jax.random.normal(key_values, (TILE_CAP, TILE, TILE), jnp.float32), -6.0, 6.0)
        kept = jax.random.uniform(key_mask, (TILE_CAP, TILE, TILE), jnp.float32) < density
        return jnp.where(kept, values * spread, 0.0).astype(jnp.bfloat16)
    return lax.map(one_block, jnp.arange(BLOCKS, dtype=jnp.int32))


def draw_tile_count(key, part):
    key_divisor, key_top = jax.random.split(jax.random.fold_in(key, 23))
    divisor = jax.random.randint(key_divisor, (BLOCKS,), 1, 5)
    counts = TILE_CAP // divisor
    chosen_top = jax.random.randint(key_top, (), 0, BLOCKS)
    return jnp.where(jnp.arange(BLOCKS) == chosen_top, TILE_CAP, counts).astype(jnp.int32)


def touch_ends(values, key, least, largest):
    longest = values.shape.index(max(values.shape))
    spots = []
    for shift in (0, 1):
        where = [jax.random.randint(jax.random.fold_in(key, axis), (), 0, length) for axis, length in enumerate(values.shape)]
        where[longest] = (where[longest] + shift) % values.shape[longest]
        spots.append(tuple(where))
    return values.at[spots[0]].set(least).at[spots[1]].set(largest)


def setup_inputs(seed: int = 0) -> dict:
    keys = jax.random.split(jax.random.key(seed), 6)
    return {
        "features": draw_features(jax.random.fold_in(keys[5], 71), 0),
        "tile_vals": draw_tile_vals(jax.random.fold_in(keys[5], 71), 0),
        "tile_cols": touch_ends(jax.random.randint(keys[2], (BLOCKS, TILE_CAP), 0, BLOCKS), jax.random.fold_in(keys[2], 1), 0, BLOCKS - 1).astype(jnp.int32),
        "tile_count": draw_tile_count(jax.random.fold_in(keys[5], 71), 0),
        "norm_gain": jnp.clip(1.0 + 0.15 * jax.random.normal(keys[4], (HOPS, WIDTH), jnp.float32), 0.25, 1.75),
    }


epsilon = 1e-05

def propagate(current, tile_vals, tile_cols, live_mask):
    blocks = current.reshape(BLOCKS, TILE, WIDTH).astype(jnp.float32)

    def one_block(inputs):
        tile_set, col_ids, live_row = inputs
        picked = blocks[col_ids.astype(jnp.int32)] * live_row[:, None, None]
        return jnp.einsum('tik,tkc->ic', tile_set.astype(jnp.float32), picked)
    return lax.map(one_block, (tile_vals, tile_cols, live_mask)).reshape(NODES, WIDTH)

def reference(features, tile_vals, tile_cols, tile_count, norm_gain):
    slot_ids = jnp.arange(TILE_CAP, dtype=jnp.int32)
    live_mask = (slot_ids[None, :] < tile_count[:, None]).astype(jnp.float32)
    current = features
    for hop_index in range(HOPS):
        summed = propagate(current, tile_vals, tile_cols, live_mask) + current.astype(jnp.float32)
        mean_sq = lax.optimization_barrier(jnp.mean(summed * summed, axis=1, keepdims=True))
        scaled = summed * lax.rsqrt(mean_sq + epsilon) * norm_gain[hop_index][None, :]
        current = scaled.astype(jnp.bfloat16)
    return current
```

```python
import functools

import jax
import jax.numpy as jnp
from jax import lax
from jax.experimental import pallas as pl
from jax.experimental.pallas import tpu as pltpu
from jax.sharding import PartitionSpec as P

epsilon = 1e-05
AXES = ("blk", "col")
CHUNK = 8


def moved(index, spots):
    result = 0
    for b, spot in enumerate(spots):
        result = result | (((index >> b) & 1) << spot)
    return result


def presum_kernel(cols_ref, count_ref, tiles_hbm, out_ref, buf, acc_a, acc_b, sems, *, devices, spots):
    slots = tiles_hbm.shape[0]
    half = out_ref.shape[2]
    chunks = slots // CHUNK
    count = count_ref[0]
    me = moved(lax.axis_index("blk") * devices[1] + lax.axis_index("col"), spots)

    def copy(c):
        window = pl.ds(c * CHUNK, CHUNK)
        return pltpu.make_async_copy(tiles_hbm.at[window], buf.at[window], sems.at[c])

    for c in range(chunks):
        @pl.when(c * CHUNK < count)
        def _():
            copy(c).start()

    def clear(i, carry):
        acc_a[i] = jnp.zeros(acc_a.shape[1:], jnp.float32)
        acc_b[i] = jnp.zeros(acc_b.shape[1:], jnp.float32)
        return carry

    lax.fori_loop(0, acc_a.shape[0], clear, 0)

    def add(acc, slot):
        @pl.when(slot < count)
        def _():
            left = me ^ moved(cols_ref[0, slot] * 2, spots)
            right = left ^ moved(1, spots)
            acc[left] = acc[left] + buf[slot, :, :half].astype(jnp.float32)
            acc[right] = acc[right] + buf[slot, :, half:].astype(jnp.float32)

    def chunk_body(c, carry):
        @pl.when(c * CHUNK < count)
        def _():
            copy(c).wait()
            for t in range(0, CHUNK, 2):
                add(acc_a, c * CHUNK + t)
                add(acc_b, c * CHUNK + t + 1)
        return carry

    lax.fori_loop(0, chunks, chunk_body, 0)

    def finish(i, carry):
        out_ref[i] = (acc_a[i] + acc_b[i]).astype(jnp.bfloat16)
        return carry

    lax.fori_loop(0, acc_a.shape[0], finish, 0)


def presum(tiles, cols, count, devices, spots):
    slots, rows, width = tiles.shape
    total = devices[0] * devices[1]
    half = width // 2
    return pl.pallas_call(
        functools.partial(presum_kernel, devices=devices, spots=spots),
        out_shape=jax.ShapeDtypeStruct((total, rows, half), jnp.bfloat16),
        in_specs=[
            pl.BlockSpec(memory_space=pltpu.SMEM),
            pl.BlockSpec(memory_space=pltpu.SMEM),
            pl.BlockSpec(memory_space=pl.ANY),
        ],
        out_specs=pl.BlockSpec(memory_space=pltpu.VMEM),
        scratch_shapes=[
            pltpu.VMEM((slots, rows, width), jnp.bfloat16),
            pltpu.VMEM((total, rows, half), jnp.float32),
            pltpu.VMEM((total, rows, half), jnp.float32),
            pltpu.SemaphoreType.DMA((slots // CHUNK,)),
        ],
        cost_estimate=pl.CostEstimate(
            flops=slots * rows * width * 8, bytes_accessed=slots * rows * width * 2, transcendentals=0
        ),
        name="presum",
    )(cols, count, tiles)


def product(adj_ref, first, parts):
    total = None
    spot = first
    for part in parts:
        blocks, rows, width = part.shape
        adj = jnp.concatenate([adj_ref[spot + j] for j in range(blocks)], axis=1)
        term = jnp.dot(adj, part[...].reshape(blocks * rows, width), preferred_element_type=jnp.float32)
        total = term if total is None else total + term
        spot += blocks
    return total


def near_kernel(adj_ref, *refs):
    refs[-1][...] = product(adj_ref, 0, refs[:-1])


def far_kernel(adj_ref, far_ref, partial_ref, own_ref, gain_ref, out_ref, *, first, hop):
    summed = product(adj_ref, first, [far_ref]) + partial_ref[...] + own_ref[...].astype(jnp.float32)
    mean_sq = jnp.mean(summed * summed, axis=1, keepdims=True)
    scaled = summed * lax.rsqrt(mean_sq + epsilon) * gain_ref[hop : hop + 1, :]
    out_ref[...] = scaled.astype(jnp.bfloat16)


def near(adj, parts):
    rows = adj.shape[1]
    width = parts[0].shape[2]
    depth = sum(part.shape[0] for part in parts) * rows
    return pl.pallas_call(
        near_kernel,
        out_shape=jax.ShapeDtypeStruct((rows, width), jnp.float32),
        cost_estimate=pl.CostEstimate(flops=2 * rows * depth * width, bytes_accessed=depth * width * 4, transcendentals=0),
        name="near",
    )(adj, *parts)


def far(adj, part, partial, own, gain, first, hop):
    return pl.pallas_call(
        functools.partial(far_kernel, first=first, hop=hop),
        out_shape=jax.ShapeDtypeStruct(own.shape, jnp.bfloat16),
        name="far",
    )(adj, part, partial, own, gain)


def exchange(value, mask, total):
    return lax.ppermute(value, AXES, [(i, i ^ mask) for i in range(total)])


def stages(devices):
    bits = (devices[0] * devices[1]).bit_length() - 1
    core_bit = devices[1].bit_length() - 1
    line = [b for b in range(bits) if b != core_bit][::-1]
    groups = [line[i : i + 2] for i in range(0, len(line), 2)]
    line = line + [core_bit]
    return groups, core_bit, [line.index(b) for b in range(bits)]


def solution(mesh):
    devices = (mesh.shape["blk"], mesh.shape["col"])
    total = devices[0] * devices[1]
    groups, core_bit, spots = stages(devices)

    def shards(features, tile_vals, tile_cols, tile_count, norm_gain):
        adj = presum(tile_vals[0], tile_cols, tile_count, devices, spots)
        current = features
        for hop in range(norm_gain.shape[0]):
            held = current[None]
            for group in groups:
                masks = [0]
                for b in group:
                    masks = masks + [m | (1 << b) for m in masks]
                parts = [held if m == 0 else exchange(held, m, total) for m in masks]
                held = jnp.concatenate(parts, axis=0)
            other = exchange(held, 1 << core_bit, total)
            partial = near(adj, [held])
            current = far(adj, other, partial, current, norm_gain, total // 2, hop)
        return current

    placed = (P(AXES, None), P("blk", None, "col", None), P("blk", None), P("blk"), P())
    return jax.shard_map(shards, mesh=mesh, in_specs=placed, out_specs=P(AXES, None), check_vma=False)
```

```python
import functools

import jax
import jax.numpy as jnp
from jax import lax
from jax.experimental import pallas as pl
from jax.experimental.pallas import tpu as pltpu
from jax.sharding import PartitionSpec as P

epsilon = 1e-05
AXES = ("blk", "col")
CHUNK = 8


def moved(index, spots):
    result = 0
    for b, spot in enumerate(spots):
        result = result ^ (((index >> b) & 1) * spot)
    return result


def presum_kernel(count_ref, cols_hbm, tiles_hbm, out_ref, cols_ref, buf, *rest, devices, spots):
    accs, sems = rest[:-1], rest[-1]
    slots = tiles_hbm.shape[0]
    rows, half = accs[0].shape[1:]
    total = out_ref.shape[0]
    chunks = slots // CHUNK
    me = moved(lax.axis_index("blk") * devices[1] + lax.axis_index("col"), spots)
    count = count_ref[0]
    cols_copy = pltpu.make_async_copy(cols_hbm, cols_ref, sems.at[chunks])

    def copy(c):
        window = pl.ds(c * CHUNK, CHUNK)
        return pltpu.make_async_copy(tiles_hbm.at[window], buf.at[window], sems.at[c])

    cols_copy.start()

    for c in range(chunks):
        @pl.when(c * CHUNK < count)
        def _():
            copy(c).start()

    def clear(i, carry):
        for acc in accs:
            acc[i] = jnp.zeros((rows, half), jnp.float32)
        return carry

    lax.fori_loop(0, total, clear, 0)
    cols_copy.wait()

    def chunk_body(c, carry):
        @pl.when(c * CHUNK < count)
        def _():
            copy(c).wait()
            for t in range(CHUNK):
                acc = accs[t % len(accs)]
                slot = c * CHUNK + t
                left = me ^ moved(cols_ref[0, slot] * 2, spots)
                right = left ^ spots[0]
                left = jnp.where(slot < count, left, total)
                right = jnp.where(slot < count, right, total + 1)
                acc[left] = acc[left] + buf[slot, :, :half].astype(jnp.float32)
                acc[right] = acc[right] + buf[slot, :, half:].astype(jnp.float32)
        return carry

    lax.fori_loop(0, chunks, chunk_body, 0)

    def finish(i, carry):
        summed = sum(acc[i] for acc in accs)
        high = summed.astype(jnp.bfloat16)
        out_ref[i, :rows] = high
        out_ref[i, rows:] = (summed - high.astype(jnp.float32)).astype(jnp.bfloat16)
        return carry

    lax.fori_loop(0, total, finish, 0)


def limit(scratch):
    return pltpu.CompilerParams(vmem_limit_bytes=scratch + 4 * 2**20)


def fast(value):
    return pltpu.with_memory_space_constraint(value, pltpu.VMEM)


def slow(value):
    return pltpu.with_memory_space_constraint(value, pltpu.HBM)


def presum(tiles, cols, count, devices, spots):
    slots, rows, width = tiles.shape
    total = devices[0] * devices[1]
    half = width // 2
    accs = [pltpu.VMEM((total + 2, rows, half), jnp.float32)] * (2 if total <= 64 else 1)
    scratch = slots * rows * width * 2 + len(accs) * (total + 2) * rows * half * 4
    return pl.pallas_call(
        functools.partial(presum_kernel, devices=devices, spots=spots),
        out_shape=pltpu.VMEM((total, 2 * rows, half), jnp.bfloat16),
        in_specs=[
            pl.BlockSpec(memory_space=pltpu.SMEM),
            pl.BlockSpec(memory_space=pltpu.HBM),
            pl.BlockSpec(memory_space=pltpu.HBM),
        ],
        out_specs=pl.BlockSpec(memory_space=pltpu.VMEM),
        scratch_shapes=[
            pltpu.SMEM((1, slots), jnp.int32),
            pltpu.VMEM((slots, rows, width), jnp.bfloat16),
            *accs,
            pltpu.SemaphoreType.DMA((slots // CHUNK + 1,)),
        ],
        cost_estimate=pl.CostEstimate(
            flops=slots * rows * width * 8, bytes_accessed=slots * rows * width * 2, transcendentals=0
        ),
        compiler_params=limit(scratch),
        name="presum",
    )(count, slow(cols), slow(tiles))


def near_kernel(value_ref, out_ref):
    out_ref[...] = value_ref[...]


def into_fast(value):
    return pl.pallas_call(
        near_kernel, out_shape=pltpu.VMEM(value.shape, value.dtype), compiler_params=limit(0), name="into_fast"
    )(slow(value))


def product(adj_ref, spots, parts):
    total = None
    for spot, part in zip(spots, parts):
        blocks, rows, width = part.shape
        adj = jnp.concatenate([adj_ref[spot + j] for j in range(blocks)], axis=1)
        term = jnp.dot(adj, part[...].reshape(blocks * rows, width), preferred_element_type=jnp.float32)
        total = term if total is None else total + term
    rows = total.shape[0] // 2
    return total[:rows] + total[rows:]


def partial_kernel(adj_ref, *refs, spots):
    refs[-1][...] = product(adj_ref, spots, refs[:-1])


def last_kernel(adj_ref, part_ref, partial_ref, own_ref, gain_ref, out_ref, *, spot, hop):
    summed = product(adj_ref, [spot], [part_ref]) + partial_ref[...] + own_ref[...].astype(jnp.float32)
    mean_sq = jnp.mean(summed * summed, axis=1, keepdims=True)
    scaled = summed * lax.rsqrt(mean_sq + epsilon) * gain_ref[hop : hop + 1, :]
    out_ref[...] = scaled.astype(jnp.bfloat16)


def partial_sum(adj, spots, parts):
    rows = adj.shape[1] // 2
    width = parts[0].shape[2]
    depth = sum(part.shape[0] for part in parts) * rows
    return pl.pallas_call(
        functools.partial(partial_kernel, spots=spots),
        out_shape=pltpu.VMEM((rows, width), jnp.float32),
        compiler_params=limit(0),
        cost_estimate=pl.CostEstimate(flops=4 * rows * depth * width, bytes_accessed=depth * width * 4, transcendentals=0),
        name="partial",
    )(fast(adj), *[fast(part) for part in parts])


def last(adj, part, partial, own, gain, spot, hop, final):
    return pl.pallas_call(
        functools.partial(last_kernel, spot=spot, hop=hop),
        out_shape=jax.ShapeDtypeStruct(own.shape, own.dtype) if final else pltpu.VMEM(own.shape, own.dtype),
        compiler_params=limit(0),
        name="last",
    )(fast(adj), fast(part), fast(partial), fast(own), fast(gain))


def exchange(value, mask, total):
    return lax.ppermute(value, AXES, [(i, i ^ mask) for i in range(total)])


def masks_of(group):
    if len(group) == 1:
        return [1 << group[0]]
    high, low = 1 << group[0], 1 << group[1]
    return [high | low, high, low]


def stages(devices):
    bits = (devices[0] * devices[1]).bit_length() - 1
    core_bit = devices[1].bit_length() - 1
    line = [b for b in range(bits) if b != core_bit][::-1]
    groups = [line[i : i + 2] for i in range(0, len(line), 2)]
    spots = [0] * bits
    size = 1
    for group in groups:
        for place, mask in enumerate(masks_of(group)):
            if mask & (mask - 1) == 0:
                spots[mask.bit_length() - 1] = size * (place + 1)
        size <<= len(group)
    spots[core_bit] = size
    return groups, core_bit, spots


def solution(mesh):
    devices = (mesh.shape["blk"], mesh.shape["col"])
    total = devices[0] * devices[1]
    groups, core_bit, spots = stages(devices)

    def shards(features, tile_vals, tile_cols, tile_count, norm_gain):
        adj = presum(tile_vals[0], tile_cols, tile_count, devices, spots)
        current = features
        for hop in range(norm_gain.shape[0]):
            held = current[None]
            if hop == 0:
                current = into_fast(current)
            for group in groups:
                received = [exchange(held, mask, total) for mask in masks_of(group)]
                parts = [current[None] if group is groups[0] else held, *received]
                if group is not groups[-1]:
                    held = jnp.concatenate(parts, axis=0)
            if hop == 0:
                *received, adj = lax.optimization_barrier((*parts[1:], adj))
                parts = [parts[0], *received]
            others = [exchange(part, 1 << core_bit, total) for part in parts]
            size = parts[0].shape[0]
            near = [j * size for j in range(len(parts))]
            far = [total // 2 + spot for spot in near]
            partial = partial_sum(adj, near + far[:-1], parts + others[:-1])
            current = last(adj, others[-1], partial, current, norm_gain, far[-1], hop, hop + 1 == norm_gain.shape[0])
        return current

    placed = (P(AXES, None), P("blk", None, "col", None), P("blk", None), P("blk"), P())
    return jax.shard_map(shards, mesh=mesh, in_specs=placed, out_specs=P(AXES, None), check_vma=False)
```

```python
import functools

import jax
import jax.numpy as jnp
from jax import lax
from jax.experimental import pallas as pl
from jax.experimental.pallas import tpu as pltpu
from jax.sharding import PartitionSpec as P

epsilon = 1e-05
AXES = ("blk", "col")
CHUNK = 8


def moved(index, spots):
    result = 0
    for b, spot in enumerate(spots):
        result = result ^ (((index >> b) & 1) * spot)
    return result


def add_tiles(count, cols_hbm, tiles_hbm, cols_ref, buf, accs, sems, window, meanwhile, devices, spots):
    first, stop = window
    half = accs[0].shape[2]
    total = devices[0] * devices[1]
    chunks = (stop - first) // CHUNK
    me = moved(lax.axis_index("blk") * devices[1] + lax.axis_index("col"), spots)
    cols_copy = pltpu.make_async_copy(cols_hbm, cols_ref, sems.at[chunks])

    def copy(c):
        return pltpu.make_async_copy(
            tiles_hbm.at[pl.ds(first + c * CHUNK, CHUNK)], buf.at[pl.ds(c * CHUNK, CHUNK)], sems.at[c]
        )

    cols_copy.start()
    for c in range(chunks):
        @pl.when(first + c * CHUNK < count)
        def _():
            copy(c).start()

    meanwhile()
    cols_copy.wait()

    def chunk_body(c, carry):
        @pl.when(first + c * CHUNK < count)
        def _():
            copy(c).wait()
            for t in range(CHUNK):
                acc = accs[t % len(accs)]
                place = c * CHUNK + t
                slot = first + place
                left = me ^ moved(cols_ref[0, slot] * 2, spots)
                right = left ^ spots[0]
                left = jnp.where(slot < count, left, total)
                right = jnp.where(slot < count, right, total + 1)
                acc[left] = acc[left] + buf[place, :, :half].astype(jnp.float32)
                acc[right] = acc[right] + buf[place, :, half:].astype(jnp.float32)
        return carry

    lax.fori_loop(0, chunks, chunk_body, 0)


def begin_kernel(count_ref, cols_hbm, tiles_hbm, own_hbm, *rest, ways, **fixed):
    own_ref, accs = rest[0], rest[1 : 1 + ways]
    cols_ref, buf, sems = rest[1 + ways :]
    own_copy = pltpu.make_async_copy(own_hbm, own_ref, sems.at[sems.shape[0] - 1])
    own_copy.start()

    def clear():
        def body(i, carry):
            for acc in accs:
                acc[i] = jnp.zeros(acc.shape[1:], jnp.float32)
            return carry

        lax.fori_loop(0, accs[0].shape[0], body, 0)

    add_tiles(count_ref[0], cols_hbm, tiles_hbm, cols_ref, buf, accs, sems, meanwhile=clear, **fixed)
    own_copy.wait()


def finish_kernel(count_ref, cols_hbm, tiles_hbm, *rest, ways, **fixed):
    out_ref, accs = rest[ways], rest[ways + 1 : 2 * ways + 1]
    cols_ref, buf, sems = rest[2 * ways + 1 :]
    rows = accs[0].shape[1]
    add_tiles(count_ref[0], cols_hbm, tiles_hbm, cols_ref, buf, accs, sems, meanwhile=lambda: None, **fixed)

    def body(i, carry):
        summed = sum(acc[i] for acc in accs)
        high = summed.astype(jnp.bfloat16)
        out_ref[i, :rows] = high
        out_ref[i, rows:] = (summed - high.astype(jnp.float32)).astype(jnp.bfloat16)
        return carry

    lax.fori_loop(0, out_ref.shape[0], body, 0)


def limit(scratch):
    return pltpu.CompilerParams(vmem_limit_bytes=scratch + 4 * 2**20)


def fast(value):
    return pltpu.with_memory_space_constraint(value, pltpu.VMEM)


def slow(value):
    return pltpu.with_memory_space_constraint(value, pltpu.HBM)


def split(slots):
    return slots * 2 // (8 * CHUNK) * CHUNK


def scratch_of(tiles, length):
    slots, rows, width = tiles.shape
    return [
        pltpu.SMEM((1, slots), jnp.int32),
        pltpu.VMEM((length, rows, width), jnp.bfloat16),
        pltpu.SemaphoreType.DMA((length // CHUNK + 2,)),
    ]


def cost_of(tiles, length):
    _, rows, width = tiles.shape
    size = length * rows * width
    return pl.CostEstimate(flops=size * 8, bytes_accessed=size * 2, transcendentals=0)


def begin(tiles, cols, count, own, devices, spots):
    slots, rows, width = tiles.shape
    total = devices[0] * devices[1]
    ways = 2 if total <= 64 else 1
    length = split(slots)
    memory = [pltpu.SMEM, pltpu.HBM, pltpu.HBM, pltpu.HBM]
    own, *accs = pl.pallas_call(
        functools.partial(begin_kernel, ways=ways, window=(0, length), devices=devices, spots=spots),
        out_shape=[pltpu.VMEM(own.shape, own.dtype)] + [pltpu.VMEM((total + 2, rows, width // 2), jnp.float32)] * ways,
        in_specs=[pl.BlockSpec(memory_space=space) for space in memory],
        out_specs=[pl.BlockSpec(memory_space=pltpu.VMEM)] * (1 + ways),
        scratch_shapes=scratch_of(tiles, length),
        cost_estimate=cost_of(tiles, length),
        compiler_params=limit(length * rows * width * 2),
        name="begin",
    )(count, slow(cols), slow(tiles), slow(own))
    return own, accs


def finish(tiles, cols, count, accs, devices, spots):
    slots, rows, width = tiles.shape
    total = devices[0] * devices[1]
    ways = len(accs)
    length = slots - split(slots)
    memory = [pltpu.SMEM, pltpu.HBM, pltpu.HBM] + [pltpu.VMEM] * ways
    return pl.pallas_call(
        functools.partial(finish_kernel, ways=ways, window=(split(slots), slots), devices=devices, spots=spots),
        out_shape=[pltpu.VMEM((total, 2 * rows, width // 2), jnp.bfloat16)] + [pltpu.VMEM(acc.shape, acc.dtype) for acc in accs],
        in_specs=[pl.BlockSpec(memory_space=space) for space in memory],
        out_specs=[pl.BlockSpec(memory_space=pltpu.VMEM)] * (1 + ways),
        input_output_aliases={3 + j: 1 + j for j in range(ways)},
        scratch_shapes=scratch_of(tiles, length),
        cost_estimate=cost_of(tiles, length),
        compiler_params=limit(length * rows * width * 2),
        name="finish",
    )(count, slow(cols), slow(tiles), *[fast(acc) for acc in accs])[0]


def product(adj_ref, spots, parts):
    total = None
    for spot, part in zip(spots, parts):
        blocks, rows, width = part.shape
        adj = jnp.concatenate([adj_ref[spot + j] for j in range(blocks)], axis=1)
        term = jnp.dot(adj, part[...].reshape(blocks * rows, width), preferred_element_type=jnp.float32)
        total = term if total is None else total + term
    rows = total.shape[0] // 2
    return total[:rows] + total[rows:]


def partial_kernel(adj_ref, *refs, spots):
    refs[-1][...] = product(adj_ref, spots, refs[:-1])


def last_kernel(adj_ref, partial_ref, own_ref, gain_ref, *refs, spots, hop):
    parts, out_ref = refs[:-1], refs[-1]
    summed = product(adj_ref, spots, parts) + partial_ref[...] + own_ref[...].astype(jnp.float32)
    mean_sq = jnp.mean(summed * summed, axis=1, keepdims=True)
    scaled = summed * lax.rsqrt(mean_sq + epsilon) * gain_ref[hop : hop + 1, :]
    out_ref[...] = scaled.astype(jnp.bfloat16)


def partial_sum(adj, spots, parts):
    rows = adj.shape[1] // 2
    width = parts[0].shape[2]
    depth = sum(part.shape[0] for part in parts) * rows
    return pl.pallas_call(
        functools.partial(partial_kernel, spots=spots),
        out_shape=pltpu.VMEM((rows, width), jnp.float32),
        compiler_params=limit(0),
        cost_estimate=pl.CostEstimate(flops=4 * rows * depth * width, bytes_accessed=depth * width * 4, transcendentals=0),
        name="partial",
    )(fast(adj), *[fast(part) for part in parts])


def last(adj, parts, partial, own, gain, spots, hop, final):
    return pl.pallas_call(
        functools.partial(last_kernel, spots=spots, hop=hop),
        out_shape=jax.ShapeDtypeStruct(own.shape, own.dtype) if final else pltpu.VMEM(own.shape, own.dtype),
        compiler_params=limit(0),
        name="last",
    )(fast(adj), fast(partial), fast(own), fast(gain), *[fast(part) for part in parts])


def exchange(value, mask, total):
    return lax.ppermute(value, AXES, [(i, i ^ mask) for i in range(total)])


def masks_of(group, closing):
    if len(group) == 1:
        return [1 << group[0]]
    high, low = 1 << group[0], 1 << group[1]
    return [high | low, high, low] if closing else [high, high | low, low]


def stages(devices):
    bits = (devices[0] * devices[1]).bit_length() - 1
    core_bit = devices[1].bit_length() - 1
    line = [b for b in range(bits) if b != core_bit][::-1]
    groups = [line[i : i + 2] for i in range(0, len(line), 2)]
    spots = [0] * bits
    size = 1
    for group in groups:
        for place, mask in enumerate(masks_of(group, group is groups[-1])):
            if mask & (mask - 1) == 0:
                spots[mask.bit_length() - 1] = size * (place + 1)
        size <<= len(group)
    spots[core_bit] = size
    return groups, core_bit, spots


def solution(mesh):
    devices = (mesh.shape["blk"], mesh.shape["col"])
    total = devices[0] * devices[1]
    groups, core_bit, spots = stages(devices)

    def shards(features, tile_vals, tile_cols, tile_count, norm_gain):
        current = features
        for hop in range(norm_gain.shape[0]):
            held = current[None]
            if hop == 0:
                current, accs = begin(tile_vals[0], tile_cols, tile_count, features, devices, spots)
            for group in groups:
                received = [exchange(held, mask, total) for mask in masks_of(group, group is groups[-1])]
                if hop == 0 and group is groups[0]:
                    received, accs = lax.optimization_barrier((received, accs))
                    adj = finish(tile_vals[0], tile_cols, tile_count, accs, devices, spots)
                parts = [current[None] if group is groups[0] else held, *received]
                if group is not groups[-1]:
                    held = jnp.concatenate(parts, axis=0)
            if hop == 0:
                *received, adj = lax.optimization_barrier((*parts[1:], adj))
                parts = [parts[0], *received]
            others = [exchange(part, 1 << core_bit, total) for part in parts]
            size = parts[0].shape[0]
            near = [j * size for j in range(len(parts))]
            far = [total // 2 + spot for spot in near]
            partial = partial_sum(adj, near + far[:-3], parts + others[:-3])
            final = hop + 1 == norm_gain.shape[0]
            current = last(adj, others[-3:], partial, current, norm_gain, far[-3:], hop, final)
        return current

    placed = (P(AXES, None), P("blk", None, "col", None), P("blk", None), P("blk"), P())
    return jax.shard_map(shards, mesh=mesh, in_specs=placed, out_specs=P(AXES, None), check_vma=False)
```

```python
import functools

import jax
import jax.numpy as jnp
from jax import lax
from jax.experimental import pallas as pl
from jax.experimental.pallas import tpu as pltpu
from jax.sharding import PartitionSpec as P

epsilon = 1e-05
AXES = ("blk", "col")
CHUNK = 8
ORDERS = (((1, 0, 2), (0, 1, 2)), ((0, 1, 2), (0, 1, 2)))
SWAP = 1


def moved(index, spots):
    result = 0
    for b, spot in enumerate(spots):
        result = result ^ (((index >> b) & 1) * spot)
    return result


def landing(me, device, plan):
    core_bit, both = plan
    index = me ^ device
    core = (device >> core_bit) & 1
    return jnp.where(core == 1, moved(index, both[1]), moved(index, both[0]))


def add_tiles(count, cols_hbm, tiles_hbm, cols_ref, buf, accs, sems, window, meanwhile, devices, plan):
    first, stop = window
    half = accs[0].shape[2]
    total = devices[0] * devices[1]
    chunks = (stop - first) // CHUNK
    me = lax.axis_index("blk") * devices[1] + lax.axis_index("col")
    cols_copy = pltpu.make_async_copy(cols_hbm, cols_ref, sems.at[chunks])

    def copy(c):
        return pltpu.make_async_copy(
            tiles_hbm.at[pl.ds(first + c * CHUNK, CHUNK)], buf.at[pl.ds(c * CHUNK, CHUNK)], sems.at[c]
        )

    cols_copy.start()
    for c in range(chunks):
        @pl.when(first + c * CHUNK < count)
        def _():
            copy(c).start()

    meanwhile()
    cols_copy.wait()

    def chunk_body(c, carry):
        @pl.when(first + c * CHUNK < count)
        def _():
            copy(c).wait()
            for t in range(CHUNK):
                acc = accs[t % len(accs)]
                place = c * CHUNK + t
                slot = first + place
                left = landing(me, cols_ref[0, slot] * 2, plan)
                right = landing(me, cols_ref[0, slot] * 2 + 1, plan)
                left = jnp.where(slot < count, left, total)
                right = jnp.where(slot < count, right, total + 1)
                acc[left] = acc[left] + buf[place, :, :half].astype(jnp.float32)
                acc[right] = acc[right] + buf[place, :, half:].astype(jnp.float32)
        return carry

    lax.fori_loop(0, chunks, chunk_body, 0)


def begin_kernel(count_ref, cols_hbm, tiles_hbm, own_hbm, *rest, ways, **fixed):
    own_ref, accs = rest[0], rest[1 : 1 + ways]
    cols_ref, buf, sems = rest[1 + ways :]
    own_copy = pltpu.make_async_copy(own_hbm, own_ref, sems.at[sems.shape[0] - 1])
    own_copy.start()

    def clear():
        def body(i, carry):
            for acc in accs:
                acc[i] = jnp.zeros(acc.shape[1:], jnp.float32)
            return carry

        lax.fori_loop(0, accs[0].shape[0], body, 0)

    add_tiles(count_ref[0], cols_hbm, tiles_hbm, cols_ref, buf, accs, sems, meanwhile=clear, **fixed)
    own_copy.wait()


def finish_kernel(count_ref, cols_hbm, tiles_hbm, *rest, ways, **fixed):
    out_ref, accs = rest[ways], rest[ways + 1 : 2 * ways + 1]
    cols_ref, buf, sems = rest[2 * ways + 1 :]
    rows = accs[0].shape[1]
    add_tiles(count_ref[0], cols_hbm, tiles_hbm, cols_ref, buf, accs, sems, meanwhile=lambda: None, **fixed)

    def body(i, carry):
        summed = sum(acc[i] for acc in accs)
        high = summed.astype(jnp.bfloat16)
        out_ref[i, :rows] = high
        out_ref[i, rows:] = (summed - high.astype(jnp.float32)).astype(jnp.bfloat16)
        return carry

    lax.fori_loop(0, out_ref.shape[0], body, 0)


def limit(scratch):
    return pltpu.CompilerParams(vmem_limit_bytes=scratch + 4 * 2**20)


def fast(value):
    return pltpu.with_memory_space_constraint(value, pltpu.VMEM)


def slow(value):
    return pltpu.with_memory_space_constraint(value, pltpu.HBM)


def split(slots):
    return slots * 2 // (8 * CHUNK) * CHUNK


def scratch_of(tiles, length):
    slots, rows, width = tiles.shape
    return [
        pltpu.SMEM((1, slots), jnp.int32),
        pltpu.VMEM((length, rows, width), jnp.bfloat16),
        pltpu.SemaphoreType.DMA((length // CHUNK + 2,)),
    ]


def cost_of(tiles, length):
    _, rows, width = tiles.shape
    size = length * rows * width
    return pl.CostEstimate(flops=size * 8, bytes_accessed=size * 2, transcendentals=0)


def begin(tiles, cols, count, own, devices, plan):
    slots, rows, width = tiles.shape
    total = devices[0] * devices[1]
    ways = 2 if total <= 64 else 1
    length = split(slots)
    memory = [pltpu.SMEM, pltpu.HBM, pltpu.HBM, pltpu.HBM]
    own, *accs = pl.pallas_call(
        functools.partial(begin_kernel, ways=ways, window=(0, length), devices=devices, plan=plan),
        out_shape=[pltpu.VMEM(own.shape, own.dtype)] + [pltpu.VMEM((total + 2, rows, width // 2), jnp.float32)] * ways,
        in_specs=[pl.BlockSpec(memory_space=space) for space in memory],
        out_specs=[pl.BlockSpec(memory_space=pltpu.VMEM)] * (1 + ways),
        scratch_shapes=scratch_of(tiles, length),
        cost_estimate=cost_of(tiles, length),
        compiler_params=limit(length * rows * width * 2),
        name="begin",
    )(count, slow(cols), slow(tiles), slow(own))
    return own, accs


def finish(tiles, cols, count, accs, devices, plan):
    slots, rows, width = tiles.shape
    total = devices[0] * devices[1]
    ways = len(accs)
    length = slots - split(slots)
    memory = [pltpu.SMEM, pltpu.HBM, pltpu.HBM] + [pltpu.VMEM] * ways
    return pl.pallas_call(
        functools.partial(finish_kernel, ways=ways, window=(split(slots), slots), devices=devices, plan=plan),
        out_shape=[pltpu.VMEM((total, 2 * rows, width // 2), jnp.bfloat16)] + [pltpu.VMEM(acc.shape, acc.dtype) for acc in accs],
        in_specs=[pl.BlockSpec(memory_space=space) for space in memory],
        out_specs=[pl.BlockSpec(memory_space=pltpu.VMEM)] * (1 + ways),
        input_output_aliases={3 + j: 1 + j for j in range(ways)},
        scratch_shapes=scratch_of(tiles, length),
        cost_estimate=cost_of(tiles, length),
        compiler_params=limit(length * rows * width * 2),
        name="finish",
    )(count, slow(cols), slow(tiles), *[fast(acc) for acc in accs])[0]


def product(adj_ref, spots, parts):
    total = None
    for spot, part in zip(spots, parts):
        blocks, rows, width = part.shape
        adj = jnp.concatenate([adj_ref[spot + j] for j in range(blocks)], axis=1)
        term = jnp.dot(adj, part[...].reshape(blocks * rows, width), preferred_element_type=jnp.float32)
        total = term if total is None else total + term
    rows = total.shape[0] // 2
    return total[:rows] + total[rows:]


def partial_kernel(adj_ref, *refs, spots):
    refs[-1][...] = product(adj_ref, spots, refs[:-1])


def last_kernel(adj_ref, partial_ref, own_ref, gain_ref, *refs, spots, hop):
    parts, out_ref = refs[:-1], refs[-1]
    summed = product(adj_ref, spots, parts) + partial_ref[...] + own_ref[...].astype(jnp.float32)
    mean_sq = jnp.mean(summed * summed, axis=1, keepdims=True)
    scaled = summed * lax.rsqrt(mean_sq + epsilon) * gain_ref[hop : hop + 1, :]
    out_ref[...] = scaled.astype(jnp.bfloat16)


def partial_sum(adj, spots, parts):
    rows = adj.shape[1] // 2
    width = parts[0].shape[2]
    depth = sum(part.shape[0] for part in parts) * rows
    return pl.pallas_call(
        functools.partial(partial_kernel, spots=spots),
        out_shape=pltpu.VMEM((rows, width), jnp.float32),
        compiler_params=limit(0),
        cost_estimate=pl.CostEstimate(flops=4 * rows * depth * width, bytes_accessed=depth * width * 4, transcendentals=0),
        name="partial",
    )(fast(adj), *[fast(part) for part in parts])


def last(adj, parts, partial, own, gain, spots, hop, final):
    return pl.pallas_call(
        functools.partial(last_kernel, spots=spots, hop=hop),
        out_shape=jax.ShapeDtypeStruct(own.shape, own.dtype) if final else pltpu.VMEM(own.shape, own.dtype),
        compiler_params=limit(0),
        name="last",
    )(fast(adj), fast(partial), fast(own), fast(gain), *[fast(part) for part in parts])


def exchange(value, masks, core_bit, total):
    return lax.ppermute(value, AXES, [(i, i ^ masks[(i >> core_bit) & 1]) for i in range(total)])


def masks_of(group, near, stage):
    if len(group) == 1:
        return [1 << group[0]]
    high, low = 1 << group[0], 1 << group[1]
    three = [high | low, high, low]
    return [three[k] for k in ORDERS[near][stage > 0]]


def stages(devices):
    bits = (devices[0] * devices[1]).bit_length() - 1
    core_bit = devices[1].bit_length() - 1
    line = [b for b in range(bits) if b != core_bit][::-1]
    groups = [line[i : i + 2] for i in range(0, len(line), 2)]
    both = []
    for core in range(2):
        order = list(groups)
        if core == SWAP and len(groups[0]) == len(groups[-1]):
            order[0], order[-1] = order[-1], order[0]
        spots = [0] * bits
        size = 1
        masks = []
        for stage, group in enumerate(order):
            masks.append(masks_of(group, group is groups[-1], stage))
            for place, mask in enumerate(masks[-1]):
                if mask & (mask - 1) == 0:
                    spots[mask.bit_length() - 1] = size * (place + 1)
            size <<= len(group)
        spots[core_bit] = size
        both.append((spots, masks))
    return [list(zip(*pair)) for pair in zip(both[0][1], both[1][1])], core_bit, [spots for spots, _ in both]


def solution(mesh):
    devices = (mesh.shape["blk"], mesh.shape["col"])
    total = devices[0] * devices[1]
    groups, core_bit, both = stages(devices)
    plan = (core_bit, both)
    swap = [1 << core_bit] * 2

    def shards(features, tile_vals, tile_cols, tile_count, norm_gain):
        current = features
        for hop in range(norm_gain.shape[0]):
            held = current[None]
            if hop == 0:
                current, accs = begin(tile_vals[0], tile_cols, tile_count, features, devices, plan)
            for group in groups:
                received = [exchange(held, masks, core_bit, total) for masks in group]
                if hop == 0 and group is groups[0]:
                    received, accs = lax.optimization_barrier((received, accs))
                    adj = finish(tile_vals[0], tile_cols, tile_count, accs, devices, plan)
                parts = [current[None] if group is groups[0] else held, *received]
                if group is not groups[-1]:
                    held = jnp.concatenate(parts, axis=0)
            if hop == 0:
                *received, adj = lax.optimization_barrier((*parts[1:], adj))
                parts = [parts[0], *received]
            others = [exchange(part, swap, core_bit, total) for part in parts]
            size = parts[0].shape[0]
            near = [j * size for j in range(len(parts))]
            far = [total // 2 + spot for spot in near]
            partial = partial_sum(adj, near + far[:-3], parts + others[:-3])
            final = hop + 1 == norm_gain.shape[0]
            current = last(adj, others[-3:], partial, current, norm_gain, far[-3:], hop, final)
        return current

    placed = (P(AXES, None), P("blk", None, "col", None), P("blk", None), P("blk"), P())
    return jax.shard_map(shards, mesh=mesh, in_specs=placed, out_specs=P(AXES, None), check_vma=False)
```
